32 devices in a mesh: data: 1 (over z), tp: 32 (over y, x, core).
Axes of the slice: x: 4, y: 4, z: 1, core: 2. Of those that a mesh axis runs over, the one named last changes fastest.
The devices are a block of a 4x4x8 slice.
Arguments:
- x: bfloat16 [8192, 8192], P('data', 'tp')
- w: bfloat16 [8192, 3072], P('tp')
- r: bfloat16 [8192, 3072], P('data')
- g: bfloat16 [3072], replicated
Outputs:
- output: bfloat16 [8192, 3072], P('data')
All inputs are finite; a program needn't handle non-finite values.
Results may differ from the reference program's by a relative error of at most 0.0117065.
Values are sent between devices in bfloat16 or wider.
A program may use at most 768 MiB of HBM per device.

```python
import jax
import jax.numpy as jnp
from jax import lax

T = 8192
H = 3072
F = 8192
EPS = 1e-6


def setup_inputs(seed: int = 0, part: int = 0) -> dict:
    kp = jax.random.fold_in(jax.random.key(seed), part)
    kx, kr = jax.random.split(kp)
    kw, kg = jax.random.split(jax.random.key(seed + 1))
    x = jax.random.normal(kx, (T, F), jnp.float32).astype(jnp.bfloat16)
    w = (jax.random.normal(kw, (F, H), jnp.float32) * (F ** -0.5)).astype(jnp.bfloat16)
    r = jax.random.normal(kr, (T, H), jnp.float32).astype(jnp.bfloat16)
    g = jax.random.uniform(kg, (H,), jnp.float32, 0.5, 1.5).astype(jnp.bfloat16)
    return {"x": x, "w": w, "r": r, "g": g}


def reference(x, w, r, g):
    y = jnp.dot(x, w, preferred_element_type=jnp.float32).astype(jnp.bfloat16)
    a = r.astype(jnp.float32) + y.astype(jnp.float32)
    ms = jnp.mean(a * a, axis=-1, keepdims=True)
    z = a * lax.rsqrt(ms + EPS) * g.astype(jnp.float32)
    return z.astype(jnp.bfloat16)
```

```python
import functools
import math

import jax
import jax.numpy as jnp
from jax import lax
from jax.experimental import pallas as pl
from jax.experimental.pallas import tpu as pltpu
from jax.sharding import PartitionSpec as P

EPS = 1e-6
CORES = 2
MESH = pl.DeviceIdType.MESH


def _place(side):
    me = lax.axis_index("tp")
    c = lax.rem(me, CORES)
    chip = lax.div(me, CORES)
    xx, yy = lax.rem(chip, side), lax.div(chip, side)
    return me, c, xx + (yy - xx) * c, yy + (xx - yy) * c


def _dev(side, c, i, j):
    return CORES * (i * (1 + (side - 1) * c) + j * (side - (side - 1) * c)) + c


def _send(src, dst, ssem, rsem, dev):
    pltpu.make_async_remote_copy(
        src_ref=src, dst_ref=dst, send_sem=ssem, recv_sem=rsem,
        device_id={"tp": dev}, device_id_type=MESH,
    ).start()


def _wait_recv(ref, sem, dev):
    pltpu.make_async_remote_copy(
        src_ref=ref, dst_ref=ref, send_sem=sem, recv_sem=sem,
        device_id={"tp": dev}, device_id_type=MESH,
    ).wait_recv()


def _wait_send(ref, sem, dev):
    pltpu.make_async_remote_copy(
        src_ref=ref, dst_ref=ref, send_sem=sem, recv_sem=sem,
        device_id={"tp": dev}, device_id_type=MESH,
    ).wait_send()


def _barrier(devs):
    bar = pltpu.get_barrier_semaphore()
    for d in devs:
        pl.semaphore_signal(bar, inc=1, device_id={"tp": d}, device_id_type=MESH)
    pl.semaphore_wait(bar, len(devs))


def _reduce_kernel(
    side, total,
    x_ref, w_ref, r_ref, g_ref, z_ref,
    wg, xl, xg, xr, acc, s2, sp, sm, ra, rb, fm, fp, rt,
    lsem, wrel, wsem, wssem, xrel, xsem, xssem, xrssem, rsem, rssem,
):
    me, c, i, j = _place(side)
    o = 1 - c
    kf = x_ref.shape[1]
    blk = z_ref.shape[0]
    half = blk // 2
    hk = kf // 2
    group = side * blk
    width = wg.shape[1]

    def at(v, d):
        return lax.rem(v + d + side, side)

    ip, im, jp, jm = at(i, 1), at(i, -1), at(j, 1), at(j, -1)
    partner = _dev(side, o, j, i)
    in_p, in_m = _dev(side, c, ip, j), _dev(side, c, im, j)
    red_p, red_m = _dev(side, c, i, jp), _dev(side, c, i, jm)
    ot_p, ot_m = _dev(side, o, jp, i), _dev(side, o, jm, i)
    from_p, from_m = _dev(side, o, j, ip), _dev(side, o, j, im)

    rows0 = c * (total // CORES) + i * group + j * blk
    cw = pltpu.make_async_copy(w_ref, wg.at[pl.ds((i * CORES + c) * kf, kf)], lsem.at[0])
    cw.start()
    cx = pltpu.make_async_copy(x_ref, xl, lsem.at[1])
    cx.start()
    cr = pltpu.make_async_copy(r_ref.at[pl.ds(rows0, blk)], rt, lsem.at[2])
    cr.start()

    _barrier((partner, in_p, in_m, red_p, red_m, ot_p, ot_m, from_p, from_m))
    cw.wait()

    own = (i * CORES + c) * kf
    oth = (j * CORES + c) * kf
    for h in (0, 1):
        src = wg.at[pl.ds(own + h * hk, hk)]
        dst_own = wg.at[pl.ds(own + h * hk, hk)]
        dst_oth = wg.at[pl.ds(oth + h * hk, hk)]
        _send(src, dst_own, wssem, wrel.at[0, c] if h == 0 else wsem, in_p)
        _send(src, dst_oth, wssem, wrel.at[0, c] if h == 0 else wsem, ot_p)
        _send(src, dst_own, wssem, wrel.at[1, c] if h == 1 else wsem, in_m)
        _send(src, dst_oth, wssem, wrel.at[1, c] if h == 1 else wsem, ot_m)
    _send(wg.at[pl.ds(own, kf)], wg.at[pl.ds(oth, kf)], wssem, wsem, partner)

    cx.wait()
    order = (2, 1, -1, 0)

    def send_x(n):
        for cc, a, b, up, down in ((c, i, j, in_p, in_m), (o, j, i, ot_p, ot_m)):
            base = cc * (total // CORES) + at(b, order[n]) * blk
            cols = pl.ds((a * CORES + c) * kf, kf)
            far = base + at(a, 2) * group
            _send(xl.at[pl.ds(far, half)], xr.at[n, 0, c], xssem, xrel.at[n, 0, c], up)
            _send(xl.at[pl.ds(far + half, half)], xr.at[n, 1, c], xssem, xrel.at[n, 1, c], down)
            _send(xl.at[pl.ds(base + at(a, 1) * group, blk)],
                  xg.at[pl.ds(n * blk, blk), cols], xssem, xsem.at[n], up)
            _send(xl.at[pl.ds(base + at(a, -1) * group, blk)],
                  xg.at[pl.ds(n * blk, blk), cols], xssem, xsem.at[n], down)
        base = o * (total // CORES) + j * group + at(i, order[n]) * blk
        _send(xl.at[pl.ds(base, blk)],
              xg.at[pl.ds(n * blk, blk), pl.ds((j * CORES + c) * kf, kf)], xssem, xsem.at[n], partner)
        base = c * (total // CORES) + i * group + at(j, order[n]) * blk
        cols = pl.multiple_of((i * CORES + c) * kf, kf)
        xg[n * blk:(n + 1) * blk, pl.ds(cols, kf)] = xl[pl.ds(pl.multiple_of(base, blk), blk), :]

    def pass_x(n):
        for e in range(CORES):
            _wait_recv(xr.at[n, 0, e], xrel.at[n, 0, e], partner)
            _send(xr.at[n, 0, e], xg.at[pl.ds(n * blk, half), pl.ds((im * CORES + e) * kf, kf)],
                  xrssem, xsem.at[n], in_p)
            _wait_recv(xr.at[n, 1, e], xrel.at[n, 1, e], partner)
            _send(xr.at[n, 1, e], xg.at[pl.ds(n * blk + half, half), pl.ds((ip * CORES + e) * kf, kf)],
                  xrssem, xsem.at[n], in_m)

    for e in range(CORES):
        slot = (im * CORES + e) * kf
        _wait_recv(wg.at[pl.ds(slot, hk)], wrel.at[0, e], partner)
        _send(wg.at[pl.ds(slot, hk)], wg.at[pl.ds(slot, hk)], wssem, wsem, in_p)
        slot = (ip * CORES + e) * kf + hk
        _wait_recv(wg.at[pl.ds(slot, hk)], wrel.at[1, e], partner)
        _send(wg.at[pl.ds(slot, hk)], wg.at[pl.ds(slot, hk)], wssem, wsem, in_m)
    for n in range(side):
        send_x(n)
    pass_x(0)
    _wait_recv(wg.at[pl.ds(0, (2 * side * CORES - 6) * hk)], wsem, partner)

    tile = next(t for t in (512, 256, 128) if width % t == 0)

    def matmul(n):
        _wait_recv(xg.at[pl.ds(n * blk, blk), pl.ds(0, (side * CORES - 1) * kf)], xsem.at[n], partner)

        @pl.loop(0, width // tile)
        def _(t):
            cols = pl.ds(pl.multiple_of(t * tile, tile), tile)
            acc[:, cols] = jnp.dot(
                xg[n * blk:(n + 1) * blk, :], wg[:, cols], preferred_element_type=jnp.float32)

    step = next(s for s in (32, 16, 8) if half % s == 0)

    def rounded(dst, first, add=None):
        @pl.loop(0, half // step)
        def _(t):
            off = pl.multiple_of(t * step, step)
            v = acc[pl.ds(first + off, step), :]
            if add is not None:
                v = v + add[pl.ds(off, step), :].astype(jnp.float32)
            dst[pl.ds(first + off, step), :] = v.astype(dst.dtype)

    lo, hi = pl.ds(0, half), pl.ds(half, half)
    matmul(0)
    rounded(s2, 0)
    _send(s2.at[lo], ra, rssem.at[0], rsem.at[0], red_p)
    rounded(s2, half)
    _send(s2.at[hi], rb, rssem.at[0], rsem.at[1], red_m)
    pass_x(1)
    matmul(1)
    rounded(sp, half)
    _send(sp.at[hi], fm.at[hi], rssem.at[1], rsem.at[2], red_p)
    pass_x(2)
    _wait_recv(ra, rsem.at[0], partner)
    rounded(sp, 0, ra)
    _send(sp.at[lo], fm.at[lo], rssem.at[1], rsem.at[2], red_p)
    matmul(2)
    rounded(sm, 0)
    _send(sm.at[lo], fp.at[lo], rssem.at[2], rsem.at[3], red_m)
    pass_x(3)
    _wait_recv(rb, rsem.at[1], partner)
    rounded(sm, half, rb)
    _send(sm.at[hi], fp.at[hi], rssem.at[2], rsem.at[3], red_m)
    matmul(3)
    cr.wait()
    _wait_recv(fm, rsem.at[2], partner)
    _wait_recv(fp, rsem.at[3], partner)

    @pl.loop(0, blk // step)
    def _(t):
        rows = pl.ds(pl.multiple_of(t * step, step), step)
        y = acc[rows, :] + (fm[rows, :].astype(jnp.float32) + fp[rows, :].astype(jnp.float32))
        a = rt[rows, :].astype(jnp.float32) + y.astype(jnp.bfloat16).astype(jnp.float32)
        ms = jnp.mean(a * a, axis=-1, keepdims=True)
        z_ref[rows, :] = (a * lax.rsqrt(ms + EPS) * g_ref[...].astype(jnp.float32)).astype(z_ref.dtype)

    _wait_send(wg.at[pl.ds(0, 7 * kf)], wssem, partner)
    _wait_send(xg.at[:, pl.ds(0, 7 * kf)], xssem, partner)
    _wait_send(xg.at[:, pl.ds(0, 2 * kf)], xrssem, partner)
    for n, ref in enumerate((s2, sp, sm)):
        _wait_send(ref, rssem.at[n], partner)


def _gather_kernel(side, zl_ref, z_ref, rsem, csem, ssem):
    me, c, i, j = _place(side)
    blk = zl_ref.shape[0]
    q = blk // 4
    base = c * (z_ref.shape[0] // CORES)
    partner = _dev(side, 1 - c, j, i)

    def at(v, d):
        return lax.rem(v + d + side, side)

    near = {
        (0, 1): _dev(side, c, at(i, 1), j), (0, -1): _dev(side, c, at(i, -1), j),
        (1, 1): _dev(side, c, i, at(j, 1)), (1, -1): _dev(side, c, i, at(j, -1)),
    }

    def offset(k, p, s):
        slot = at(i, k[0]) * side + at(j, k[1])
        return base + slot * blk + (2 * p + s) * q, slot * 4 + 2 * p + s

    own = base + (i * side + j) * blk

    @pl.loop(0, blk // 8)
    def _(t):
        row = pl.multiple_of(t * 8, 8)
        z_ref[pl.ds(pl.multiple_of(own + row, 8), 8), :] = zl_ref[pl.ds(row, 8), :]

    _barrier((partner,) + tuple(near.values()))

    def ship(k, p, s, ways):
        off, slot = offset(k, p, s)
        piece = z_ref.at[pl.ds(off, q)]
        for way in ways:
            _send(piece, piece, ssem, rsem.at[slot], near[way])
        _send(piece, piece, ssem, csem, partner)

    def take(k, p, s, ways):
        off, slot = offset(k, p, s)
        _wait_recv(z_ref.at[pl.ds(off, q)], rsem.at[slot], partner)
        ship(k, p, s, ways)

    def vec(p, d, e=0):
        return (d, e) if p == 0 else (e, d)

    both = lambda axis: ((axis, 1), (axis, -1))
    for p in (0, 1):
        for s in (0, 1):
            off, slot = offset((0, 0), p, s)
            piece = z_ref.at[pl.ds(off, q)]
            for way in both(p):
                _send(piece, piece, ssem, rsem.at[slot], near[way])
    for p in (0, 1):
        for s in (0, 1):
            ship((0, 0), p, s, both(1 - p))
    for s in (0, 1):
        for p in (0, 1):
            for d in (-1, 1):
                on = ((p, -d),) if (s == 0) == (d == -1) else ()
                take(vec(p, d), p, s, on + both(1 - p))
    def second(d1):
        for s in (0, 1):
            for p in (0, 1):
                for d in (-1, 1):
                    on = ((1 - p, -d),) if (s == 0) == (d == -1) else ()
                    take(vec(p, d1, d), p, s, on)
    second(0)
    for s in (0, 1):
        for p in (0, 1):
            take(vec(p, 2), p, s, both(1 - p))
    second(-1)
    second(1)
    second(2)
    for d1 in (0, -1, 1, 2):
        for s in (0, 1):
            for p in (0, 1):
                take(vec(p, d1, 2), p, s, ())
    n = side * side * 4
    _wait_recv(z_ref.at[pl.ds(0, n * q)], csem, partner)
    _wait_send(z_ref.at[pl.ds(0, (2 * n - 4) * q)], ssem, partner)


def _store_kernel(z_ref, o_ref, sem):
    copy = pltpu.make_async_copy(z_ref, o_ref, sem)
    copy.start()
    copy.wait()


def solution(mesh):
    tp = mesh.shape["tp"]
    side = math.isqrt(tp // CORES)

    def local(x, w, r, g):
        total, kf = x.shape
        width = w.shape[1]
        blk = total // tp
        bf = jnp.bfloat16
        dma = pltpu.SemaphoreType.DMA
        any_ = pl.BlockSpec(memory_space=pl.ANY)
        vmem = pl.BlockSpec(memory_space=pltpu.VMEM)
        zl = pl.pallas_call(
            functools.partial(_reduce_kernel, side, total),
            out_shape=pltpu.VMEM((blk, width), bf),
            in_specs=[any_, any_, any_, vmem],
            out_specs=vmem,
            scratch_shapes=[
                pltpu.VMEM((side * CORES * kf, width), bf),
                pltpu.VMEM((total, kf), bf),
                pltpu.VMEM((side * blk, side * CORES * kf), bf),
                pltpu.VMEM((side, 2, CORES, blk // 2, kf), bf),
                pltpu.VMEM((blk, width), jnp.float32),
                pltpu.VMEM((blk, width), bf),
                pltpu.VMEM((blk, width), bf),
                pltpu.VMEM((blk, width), bf),
                pltpu.VMEM((blk // 2, width), bf),
                pltpu.VMEM((blk // 2, width), bf),
                pltpu.VMEM((blk, width), bf),
                pltpu.VMEM((blk, width), bf),
                pltpu.VMEM((blk, width), bf),
                dma((3,)), dma((2, CORES)), dma, dma,
                dma((side, 2, CORES)), dma((side,)), dma, dma,
                dma((4,)), dma((3,)),
            ],
            compiler_params=pltpu.CompilerParams(
                collective_id=0, has_side_effects=True, vmem_limit_bytes=56 * 2**20),
            name="reduce",
        )(x, w, r, g.reshape(1, width))
        z = pl.pallas_call(
            functools.partial(_gather_kernel, side),
            out_shape=pltpu.VMEM(r.shape, bf),
            in_specs=[vmem],
            out_specs=vmem,
            scratch_shapes=[dma((side * side * 4,)), dma, dma],
            compiler_params=pltpu.CompilerParams(
                collective_id=1, has_side_effects=True, vmem_limit_bytes=4 * 2**20),
            name="gather",
        )(zl)
        return pl.pallas_call(
            _store_kernel,
            out_shape=pltpu.HBM(r.shape, bf),
            in_specs=[vmem],
            out_specs=pl.BlockSpec(memory_space=pltpu.HBM),
            scratch_shapes=[dma],
            compiler_params=pltpu.CompilerParams(vmem_limit_bytes=2**20),
            name="store",
        )(z)

    return jax.shard_map(
        local,
        mesh=mesh,
        in_specs=(P("data", "tp"), P("tp", None), P("data", None), P(None)),
        out_specs=P("data", None),
        check_vma=False,
    )
```

```python
import functools
import math

import jax
import jax.numpy as jnp
from jax import lax
from jax.experimental import pallas as pl
from jax.experimental.pallas import tpu as pltpu
from jax.sharding import PartitionSpec as P

EPS = 1e-6
CORES = 2
MESH = pl.DeviceIdType.MESH


def _place(side):
    me = lax.axis_index("tp")
    c = lax.rem(me, CORES)
    chip = lax.div(me, CORES)
    xx, yy = lax.rem(chip, side), lax.div(chip, side)
    return me, c, xx + (yy - xx) * c, yy + (xx - yy) * c


def _dev(side, c, i, j):
    return CORES * (i * (1 + (side - 1) * c) + j * (side - (side - 1) * c)) + c


def _send(src, dst, ssem, rsem, dev):
    pltpu.make_async_remote_copy(
        src_ref=src, dst_ref=dst, send_sem=ssem, recv_sem=rsem,
        device_id={"tp": dev}, device_id_type=MESH,
    ).start()


def _wait_recv(ref, sem, dev):
    pltpu.make_async_remote_copy(
        src_ref=ref, dst_ref=ref, send_sem=sem, recv_sem=sem,
        device_id={"tp": dev}, device_id_type=MESH,
    ).wait_recv()


def _wait_send(ref, sem, dev):
    pltpu.make_async_remote_copy(
        src_ref=ref, dst_ref=ref, send_sem=sem, recv_sem=sem,
        device_id={"tp": dev}, device_id_type=MESH,
    ).wait_send()


def _barrier(devs):
    bar = pltpu.get_barrier_semaphore()
    for d in devs:
        pl.semaphore_signal(bar, inc=1, device_id={"tp": d}, device_id_type=MESH)
    pl.semaphore_wait(bar, len(devs))


def _fused_kernel(
    side, x_ref, w_ref, r_ref, g_ref, z_ref,
    xg, xr, acc, held,
    lsem, wrel, wsem, wssem, xrel, xsem, xssem, xrssem, rsem, rssem, credit, gsem, csem, gssem,
):
    me, c, i, j = _place(side)
    o = 1 - c
    total, width = z_ref.shape
    kf = x_ref.shape[-1]
    blk = x_ref.shape[3]
    q = blk // side
    hq = q // 2
    hk = kf // 2
    hs = side // 2
    f32 = jnp.float32

    def at(v, d):
        return lax.rem(v + d + side, side)

    ip, im, jp, jm = at(i, 1), at(i, -1), at(j, 1), at(j, -1)
    partner = _dev(side, o, j, i)
    in_p, in_m = _dev(side, c, ip, j), _dev(side, c, im, j)
    red_p, red_m = _dev(side, c, i, jp), _dev(side, c, i, jm)
    ot_p, ot_m = _dev(side, o, jp, i), _dev(side, o, jm, i)
    from_p, from_m = _dev(side, o, j, ip), _dev(side, o, j, im)

    lent, mine = o * (total // CORES), c * (total // CORES)
    own_rows = mine + (i * side + j) * blk
    names = ("s2", "sp", "sm", "fm", "fp", "ra", "rb")
    where = {k: side * CORES * kf + n * blk for n, k in enumerate(names)}

    def wrows(cc, slot, first, size):
        return z_ref.at[pl.ds((1 - cc) * (total // CORES) + slot * kf + first, size)]

    def buf(k, n, first, size):
        return pl.ds(lent + where[k] + n * q + first, size)

    own, oth = i * CORES + c, j * CORES + c
    cw = pltpu.make_async_copy(w_ref, wrows(c, own, 0, kf), lsem.at[0])
    cw.start()
    cr = pltpu.make_async_copy(r_ref.at[pl.ds(own_rows, blk)], z_ref.at[pl.ds(own_rows, blk)], lsem.at[1])
    cr.start()
    cols_own = pl.ds(own * kf, kf)
    cx = [pltpu.make_async_copy(x_ref.at[c, i, :, pl.ds(n * q, q)], xg.at[n, :, :, cols_own], lsem.at[2 + n])
          for n in range(side)]
    for copy in cx:
        copy.start()

    _barrier((partner, in_p, in_m, red_p, red_m, ot_p, ot_m, from_p, from_m))
    cw.wait()

    for h in (0, 1):
        for up in (1, 0):
            src = wrows(c, own, (h if up else 1 - h) * hk, hk)
            sem = wrel.at[1 - up, c] if h == 0 else wsem
            for cc, slot, dev in ((c, own, in_p if up else in_m), (o, oth, ot_p if up else ot_m)):
                _send(src, wrows(cc, slot, (h if up else 1 - h) * hk, hk), wssem, sem, dev)
    _send(wrows(c, own, 0, kf), wrows(o, oth, 0, kf), wssem, wsem, partner)

    def send_x(n):
        rows = pl.ds(n * q, q)
        for cc, a, up, down in ((c, i, in_p, in_m), (o, j, ot_p, ot_m)):
            cols = pl.ds((a * CORES + c) * kf, kf)
            far = at(a, 2)
            _send(x_ref.at[cc, far, pl.ds(0, hs), rows], xr.at[n, 0, c], xssem, xrel.at[n, 0, c], up)
            _send(x_ref.at[cc, far, pl.ds(hs, hs), rows], xr.at[n, 1, c], xssem, xrel.at[n, 1, c], down)
            _send(x_ref.at[cc, at(a, 1), :, rows], xg.at[n, :, :, cols], xssem, xsem.at[n], up)
            _send(x_ref.at[cc, at(a, -1), :, rows], xg.at[n, :, :, cols], xssem, xsem.at[n], down)
        _send(x_ref.at[o, j, :, rows], xg.at[n, :, :, pl.ds(oth * kf, kf)], xssem, xsem.at[n], partner)

    def pass_x(n):
        for e in range(CORES):
            _wait_recv(xr.at[n, 0, e], xrel.at[n, 0, e], partner)
            _send(xr.at[n, 0, e], xg.at[n, pl.ds(0, hs), :, pl.ds((im * CORES + e) * kf, kf)],
                  xrssem, xsem.at[n], in_p)
            _wait_recv(xr.at[n, 1, e], xrel.at[n, 1, e], partner)
            _send(xr.at[n, 1, e], xg.at[n, pl.ds(hs, hs), :, pl.ds((ip * CORES + e) * kf, kf)],
                  xrssem, xsem.at[n], in_m)

    for e in range(CORES):
        for d, src, dev, first in ((0, im, in_p, 0), (1, ip, in_m, hk)):
            piece = wrows(c, src * CORES + e, first, hk)
            _wait_recv(piece, wrel.at[d, e], partner)
            _send(piece, piece, wssem, wsem, dev)
    send_x(0)
    send_x(1)

    tile = next(t for t in (512, 256, 128) if width % t == 0)
    step = next(t for t in (32, 16, 8) if hq % t == 0)
    depth = side * CORES * kf

    def matmul(n):
        cx[n].wait()
        _wait_recv(xg.at[n, :, :, pl.ds(0, depth - kf)], xsem.at[n], partner)
        w_rows = pl.ds(pl.multiple_of(lent, blk), depth)

        @pl.loop(0, width // tile)
        def _(t):
            cols = pl.ds(pl.multiple_of(t * tile, tile), tile)
            acc[n % 2, :, cols] = jnp.dot(
                xg[n].reshape(side * q, depth), z_ref[w_rows, cols], preferred_element_type=f32)

    def part(n, block, first):
        return acc.at[n % 2, pl.ds(pl.multiple_of(block * q, q) + first, hq)]

    def send_part(n, k, block, first, add, dst, sem, dev):
        src, at_ = part(n, block, first), lent + where[k] + n * q + first

        @pl.loop(0, hq // step)
        def _(t):
            off = pl.multiple_of(t * step, step)
            v = src[pl.ds(off, step), :]
            if add is not None:
                row = lent + where[add] + n * q
                v = v + z_ref[pl.ds(pl.multiple_of(row + off, step), step), :].astype(f32)
            z_ref[pl.ds(pl.multiple_of(at_ + off, step), step), :] = v.astype(z_ref.dtype)

        to = 0 if dst in ("ra", "rb") else first
        _send(z_ref.at[pl.ds(at_, hq)], z_ref.at[buf(dst, n, to, hq)], rssem, sem, dev)

    def first_hop(n):
        send_part(n, "s2", at(j, 2), 0, None, "ra", rsem.at[n, 0], red_p)
        send_part(n, "s2", at(j, 2), hq, None, "rb", rsem.at[n, 1], red_m)
        send_part(n, "sp", jp, hq, None, "fm", rsem.at[n, 2], red_p)
        send_part(n, "sm", jm, 0, None, "fp", rsem.at[n, 3], red_m)

    def keep(n):
        src, dst = acc.at[n % 2, pl.ds(pl.multiple_of(j * q, q), q)], held.at[n % 3]

        @pl.loop(0, q // 8)
        def _(t):
            rows = pl.ds(pl.multiple_of(t * 8, 8), 8)
            dst[rows, :] = src[rows, :]

    def second_hop(n):
        _wait_recv(z_ref.at[buf("ra", n, 0, hq)], rsem.at[n, 0], partner)
        send_part(n, "sp", jp, 0, "ra", "fm", rsem.at[n, 2], red_p)
        _wait_recv(z_ref.at[buf("rb", n, 0, hq)], rsem.at[n, 1], partner)
        send_part(n, "sm", jm, hq, "rb", "fp", rsem.at[n, 3], red_m)

    near = {(0, 1): in_p, (0, -1): in_m, (1, 1): red_p, (1, -1): red_m}

    def piece_of(k, n):
        slot = at(i, k[0]) * side + at(j, k[1])
        return z_ref.at[pl.ds(mine + slot * blk + n * q, q)], slot * side + n

    def both(axis):
        return (axis, 1), (axis, -1)

    def norm(n):
        if n == 0:
            cr.wait()
        _wait_recv(z_ref.at[buf("fm", n, 0, q)], rsem.at[n, 2], partner)
        _wait_recv(z_ref.at[buf("fp", n, 0, q)], rsem.at[n, 3], partner)
        src = held.at[n % 3]

        @pl.loop(0, q // step)
        def _(t):
            off = pl.multiple_of(t * step, step)

            def rows(first):
                return pl.ds(pl.multiple_of(first + n * q + off, step), step)

            y = src[pl.ds(off, step), :] + (
                z_ref[rows(lent + where["fm"]), :].astype(f32) + z_ref[rows(lent + where["fp"]), :].astype(f32))
            a = z_ref[rows(own_rows), :].astype(f32) + y.astype(z_ref.dtype).astype(f32)
            ms = jnp.mean(a * a, axis=-1, keepdims=True)
            z_ref[rows(own_rows), :] = (
                a * lax.rsqrt(ms + EPS) * g_ref[...].astype(f32).reshape(1, width)).astype(z_ref.dtype)

        piece, slot = piece_of((0, 0), n)
        for way in both(n % 2) + both(1 - n % 2):
            _send(piece, piece, gssem, gsem.at[slot], near[way])

    pass_x(0)
    send_x(2)
    pass_x(1)
    send_x(3)
    _wait_recv(z_ref.at[pl.ds(lent, (2 * side * CORES - 6) * hk)], wsem, partner)
    for n in range(side):
        matmul(n)
        first_hop(n)
        keep(n)
        if n + 2 < side:
            pass_x(n + 2)
        if n > 0:
            second_hop(n - 1)
        if n > 1:
            norm(n - 2)
    second_hop(side - 1)
    norm(side - 2)
    norm(side - 1)

    kept = [((0, 0), n) for n in range(side)]

    def take(k, n, ways):
        piece, slot = piece_of(k, n)
        _wait_recv(piece, gsem.at[slot], partner)
        for way in ways:
            _send(piece, piece, gssem, gsem.at[slot], near[way])
        if kept is None:
            _send(piece, piece, gssem, csem, partner)
        else:
            kept.append((k, n))

    def vec(n, d, e=0):
        return (d, e) if n % 2 == 0 else (e, d)

    def onward(n, axis, d):
        return ((axis, -d),) if (n < 2) == (d == -1) else ()

    def second(d1):
        for n in range(side):
            for d in (-1, 1):
                take(vec(n, d1, d), n, onward(n, 1 - n % 2, d))

    def far(d1):
        for n in range(side):
            take(vec(n, d1, 2), n, ())

    for n in range(side):
        for d in (-1, 1):
            take(vec(n, d), n, onward(n, n % 2, d) + both(1 - n % 2))

    _wait_send(z_ref.at[pl.ds(lent, 7 * kf)], wssem, partner)
    _wait_send(z_ref.at[pl.ds(lent, 3 * blk)], rssem, partner)
    pl.semaphore_signal(credit, inc=1, device_id={"tp": partner}, device_id_type=MESH)
    second(0)
    for n in range(side):
        take(vec(n, 2), n, both(1 - n % 2))
    pl.semaphore_wait(credit, 1)
    for k, n in kept:
        piece, _ = piece_of(k, n)
        _send(piece, piece, gssem, csem, partner)
    kept = None
    second(-1)
    second(1)
    far(0)
    second(2)
    far(-1)
    far(1)
    far(2)
    count = side * side * side
    _wait_recv(z_ref.at[pl.ds(0, count * q)], csem, partner)
    _wait_send(z_ref.at[pl.ds(0, (2 * count - side) * q)], gssem, partner)
    _wait_send(xg.at[:, :, :, pl.ds(0, depth - kf)], xssem, partner)
    _wait_send(xg.at[:, :, :, pl.ds(0, 2 * kf)], xrssem, partner)


def _store_kernel(z_ref, o_ref, sem):
    n = 16
    rows = z_ref.shape[0] // n
    cs = [pltpu.make_async_copy(z_ref.at[pl.ds(k * rows, rows)], o_ref.at[pl.ds(k * rows, rows)], sem.at[k]) for k in range(n)]
    for c in cs:
        c.start()
    for c in cs:
        c.wait()


def solution(mesh):
    tp = mesh.shape["tp"]
    side = math.isqrt(tp // CORES)

    def local(x, w, r, g):
        total, kf = x.shape
        width = w.shape[1]
        blk = total // tp
        bf = jnp.bfloat16
        dma = pltpu.SemaphoreType.DMA
        any_ = pl.BlockSpec(memory_space=pl.ANY)
        vmem = pl.BlockSpec(memory_space=pltpu.VMEM)
        z = pl.pallas_call(
            functools.partial(_fused_kernel, side),
            out_shape=pltpu.VMEM(r.shape, bf),
            in_specs=[any_, any_, any_, vmem],
            out_specs=vmem,
            scratch_shapes=[
                pltpu.VMEM((side, side, blk // side, side * CORES * kf), bf),
                pltpu.VMEM((side, 2, CORES, side // 2, blk // side, kf), bf),
                pltpu.VMEM((2, blk, width), jnp.float32),
                pltpu.VMEM((3, blk // side, width), jnp.float32),
                dma((2 + side,)), dma((2, CORES)), dma, dma,
                dma((side, 2, CORES)), dma((side,)), dma, dma,
                dma((side, 4)), dma, pltpu.SemaphoreType.REGULAR,
                dma((side * side * side,)), dma, dma,
            ],
            compiler_params=pltpu.CompilerParams(
                collective_id=0, has_side_effects=True, vmem_limit_bytes=63 * 2**18),
            name="fused",
        )(x.reshape(CORES, side, side, blk, kf), w, r, g)
        return pl.pallas_call(
            _store_kernel,
            out_shape=pltpu.HBM(r.shape, bf),
            in_specs=[vmem],
            out_specs=pl.BlockSpec(memory_space=pltpu.HBM),
            scratch_shapes=[dma((16,))],
            compiler_params=pltpu.CompilerParams(vmem_limit_bytes=2**20),
            name="store",
        )(z)

    return jax.shard_map(
        local,
        mesh=mesh,
        in_specs=(P("data", "tp"), P("tp", None), P("data", None), P(None)),
        out_specs=P("data", None),
        check_vma=False,
    )
```

```python
import functools
import math

import jax
import jax.numpy as jnp
from jax import lax
from jax.experimental import pallas as pl
from jax.experimental.pallas import tpu as pltpu
from jax.sharding import PartitionSpec as P

EPS = 1e-6
CORES = 2
MESH = pl.DeviceIdType.MESH


def _place(side):
    me = lax.axis_index("tp")
    c = lax.rem(me, CORES)
    chip = lax.div(me, CORES)
    xx, yy = lax.rem(chip, side), lax.div(chip, side)
    return me, c, xx + (yy - xx) * c, yy + (xx - yy) * c


def _dev(side, c, i, j):
    return CORES * (i * (1 + (side - 1) * c) + j * (side - (side - 1) * c)) + c


def _send(src, dst, ssem, rsem, dev):
    pltpu.make_async_remote_copy(
        src_ref=src, dst_ref=dst, send_sem=ssem, recv_sem=rsem,
        device_id={"tp": dev}, device_id_type=MESH,
    ).start()


def _wait_recv(ref, sem, dev):
    pltpu.make_async_remote_copy(
        src_ref=ref, dst_ref=ref, send_sem=sem, recv_sem=sem,
        device_id={"tp": dev}, device_id_type=MESH,
    ).wait_recv()


def _wait_send(ref, sem, dev):
    pltpu.make_async_remote_copy(
        src_ref=ref, dst_ref=ref, send_sem=sem, recv_sem=sem,
        device_id={"tp": dev}, device_id_type=MESH,
    ).wait_send()


def _barrier(devs):
    bar = pltpu.get_barrier_semaphore()
    for d in devs:
        pl.semaphore_signal(bar, inc=1, device_id={"tp": d}, device_id_type=MESH)
    pl.semaphore_wait(bar, len(devs))


def _fused_kernel(
    side, x_ref, w_ref, r_ref, g_ref, z_ref,
    xo, acc, held, gain, sums, stat_out, stat_in,
    lsem, wrel, wsem, wssem, xrel, xsem, xssem, xrssem, rsem, rssem, tsem, tssem, credit, gsem, csem, gssem,
):
    me, c, i, j = _place(side)
    o = 1 - c
    halves, groups, q, hw = z_ref.shape
    width = halves * hw
    kf = x_ref.shape[-1]
    hq = q // 2
    kg = kf // q
    per_core = groups // CORES
    f32 = jnp.float32
    bf = z_ref.dtype

    def at(v, d):
        return lax.rem(v + d + side, side)

    def nh(a):
        return lax.div(a, side // 2)

    def mh(a):
        return lax.rem(lax.div(a + 1, 2), 2)

    def near_n(a):
        return a + 1 - 2 * lax.rem(a, 2)

    def near_m(a):
        return at(a, 2 * lax.rem(a, 2) - 1)

    jp, jm = at(j, 1), at(j, -1)
    partner = _dev(side, o, j, i)
    in_p, in_m = _dev(side, c, at(i, 1), j), _dev(side, c, at(i, -1), j)
    red_p, red_m = _dev(side, c, i, jp), _dev(side, c, i, jm)
    lines = []
    for cc, a, b in ((c, i, j), (o, j, i)):
        lines.append((cc, a, _dev(side, cc, near_n(a), b), _dev(side, cc, near_m(a), b)))
    from_p, from_m = _dev(side, o, j, at(i, 1)), _dev(side, o, j, at(i, -1))
    to_n, to_m = lines[0][2:]

    def cols_of(h):
        return pl.ds(pl.multiple_of(h * hw, hw), hw)

    def lent(cc, half, first, size):
        return half, pl.ds((1 - cc) * per_core + first, size)

    def w_at(cc, role, core):
        h, g = lent(cc, 0, (role * CORES + core) * kg, kg)
        return z_ref.at[h, g]

    x_first = side * CORES * kg

    def x_at(cc, n, role, core):
        if role == 3:
            return xo.at[n, :, :, pl.ds(core * kf, kf)]
        h, g = lent(cc, 0, x_first + n * side, side)
        return z_ref.at[h, g, :, pl.ds((role * CORES + core) * kf, kf)]

    names = ("s2", "sp", "sm", "fm", "fp", "ra", "rb")
    base = o * per_core

    def buf(k, n):
        return base + names.index(k) * side + n

    def own_group(ii, jj):
        return nh(ii), ((c * 2 + mh(ii)) * side + jj) * side

    my_half, my_group = own_group(i, j)

    cw = pltpu.make_async_copy(w_ref.at[:, :, cols_of(nh(i))], w_at(c, 0, c), lsem.at[0])
    cw.start()
    cr = pltpu.make_async_copy(
        r_ref.at[pl.ds(my_group, side), :, cols_of(nh(i))], z_ref.at[my_half, pl.ds(my_group, side)], lsem.at[1])
    cr.start()
    cx = [pltpu.make_async_copy(x_ref.at[c, mh(i), :, pl.ds(n * q, q)], x_at(c, n, 0, c), lsem.at[2 + n])
          for n in range(side)]
    for copy in cx:
        copy.start()

    _barrier((partner, in_p, in_m, red_p, red_m, lines[1][2], lines[1][3], from_p, from_m))

    for cc, a, dev_n, dev_m in lines:
        _send(w_ref.at[:, :, cols_of(1 - nh(a))], w_at(cc, 2, c), wssem, wrel.at[c], dev_m)
    for cc, a, dev_n, dev_m in lines:
        _send(w_ref.at[:, :, cols_of(nh(a))], w_at(cc, 1, c), wssem, wsem, dev_n)
    _send(w_ref.at[:, :, cols_of(nh(j))], w_at(o, 0, c), wssem, wsem, partner)

    def send_x(n):
        rows = pl.ds(n * q, q)
        for cc, a, dev_n, dev_m in lines:
            _send(x_ref.at[cc, mh(a), :, rows], x_at(cc, n, 2, c), xssem, xsem.at[n], dev_m)
        _send(x_ref.at[o, mh(j), :, rows], x_at(o, n, 0, c), xssem, xsem.at[n], partner)

    def relay_x(n, line):
        cc, a, dev_n, dev_m = line
        _send(x_ref.at[cc, 1 - mh(a), :, pl.ds(n * q, q)], x_at(cc, n, 1, c), xssem, xrel.at[n, c], dev_n)

    def pass_x(n):
        for e in range(CORES):
            piece = x_at(c, n, 1, e)
            _wait_recv(piece, xrel.at[n, e], partner)
            _send(piece, x_at(c, n, 3, e), xrssem, xsem.at[n], to_m)

    for n in range(side):
        send_x(n)

    gain[...] = jnp.where(
        my_half == 0, g_ref[...].astype(f32).reshape(1, width)[:, :hw], g_ref[...].astype(f32).reshape(1, width)[:, hw:])

    for line in lines:
        relay_x(0, line)
    for e in range(CORES):
        piece = w_at(c, 2, e)
        _wait_recv(piece, wrel.at[e], partner)
        _send(piece, w_at(c, 3, e), wssem, wsem, to_n)
    for line in lines:
        relay_x(1, line)
    pass_x(0)
    for line in lines:
        relay_x(2, line)
    pass_x(1)
    for line in lines:
        relay_x(3, line)
    _wait_recv(z_ref.at[0, pl.ds(base, 5 * kg)], wsem, partner)
    cw.wait()

    tile = next(t for t in (512, 256, 128) if hw % t == 0)
    step = next(t for t in (32, 16, 8) if hq % t == 0)
    roles = 3 * CORES

    def x_wait_ref(first, size, pieces):
        return z_ref.at[0, pl.ds(base + x_first + first, size), :, pl.ds(0, pieces * kf)]

    def matmul(n):
        cx[n].wait()
        _wait_recv(x_wait_ref(n * side, side, 5), xsem.at[n], partner)

        @pl.loop(0, hw // tile)
        def _(t):
            cols = pl.ds(pl.multiple_of(t * tile, tile), tile)
            near = jnp.dot(
                z_ref[0, pl.ds(base + x_first + n * side, side), :, pl.ds(0, roles * kf)].reshape(side * q, roles * kf),
                z_ref[0, pl.ds(base, roles * kg), :, cols].reshape(roles * kf, tile), preferred_element_type=f32)
            acc[n % 2, :, cols] = near + jnp.dot(
                xo[n].reshape(side * q, CORES * kf),
                z_ref[0, pl.ds(base + roles * kg, CORES * kg), :, cols].reshape(CORES * kf, tile),
                preferred_element_type=f32)

    def part(n, block, first, size):
        return acc.at[n % 2, pl.ds(pl.multiple_of(block * q, q) + first, size)]

    def send_part(n, k, block, first, add, dst, sem, dev):
        src = part(n, block, first, hq)

        @pl.loop(0, hq // step)
        def _(t):
            off = pl.multiple_of(t * step, step)
            v = src[pl.ds(off, step), :]
            if add is not None:
                v = v + z_ref[1, buf(add, n), pl.ds(off, step), :].astype(f32)
            z_ref[1, buf(k, n), pl.ds(first + off, step), :] = v.astype(bf)

        to = 0 if dst in ("ra", "rb") else first
        _send(z_ref.at[1, buf(k, n), pl.ds(first, hq)], z_ref.at[1, buf(dst, n), pl.ds(to, hq)], rssem, sem, dev)

    def first_hop(n):
        send_part(n, "s2", at(j, 2), 0, None, "ra", rsem.at[n, 0], red_p)
        send_part(n, "s2", at(j, 2), hq, None, "rb", rsem.at[n, 1], red_m)
        send_part(n, "sp", jp, hq, None, "fm", rsem.at[n, 2], red_p)
        send_part(n, "sm", jm, 0, None, "fp", rsem.at[n, 3], red_m)
        src = part(n, j, 0, q)

        @pl.loop(0, q // step)
        def _(t):
            rows = pl.ds(pl.multiple_of(t * step, step), step)
            held[n, rows, :] = src[rows, :]

    def second_hop(n):
        _wait_recv(z_ref.at[1, buf("ra", n), pl.ds(0, hq)], rsem.at[n, 0], partner)
        send_part(n, "sp", jp, 0, "ra", "fm", rsem.at[n, 2], red_p)
        _wait_recv(z_ref.at[1, buf("rb", n), pl.ds(0, hq)], rsem.at[n, 1], partner)
        send_part(n, "sm", jm, hq, "rb", "fp", rsem.at[n, 3], red_m)

    def add_up(n):
        if n == 0:
            cr.wait()
        _wait_recv(z_ref.at[1, buf("fm", n)], rsem.at[n, 2], partner)
        _wait_recv(z_ref.at[1, buf("fp", n)], rsem.at[n, 3], partner)

        @pl.loop(0, q // step)
        def _(t):
            rows = pl.ds(pl.multiple_of(t * step, step), step)
            y = held[n, rows, :] + (
                z_ref[1, buf("fm", n), rows, :].astype(f32) + z_ref[1, buf("fp", n), rows, :].astype(f32))
            v = z_ref[my_half, my_group + n, rows, :].astype(f32) + y.astype(bf).astype(f32)
            held[n, rows, :] = v
            sums[n, rows, :] = jnp.broadcast_to(jnp.sum(v * v, axis=-1, keepdims=True), (step, sums.shape[-1]))

        stat_out[n] = sums[n].T[:8]
        _send(stat_out.at[n], stat_in.at[n], tssem, tsem.at[n], to_m)

    near = {(0, 1): in_p, (0, -1): in_m, (1, 1): red_p, (1, -1): red_m}

    def piece_of(k, n):
        ii, jj = at(i, k[0]), at(j, k[1])
        h, g = own_group(ii, jj)
        return z_ref.at[h, g + n], (ii * side + jj) * side + n

    def both(axis):
        return (axis, 1), (axis, -1)

    def norm(n):
        _wait_recv(stat_in.at[n], tsem.at[n], partner)
        theirs = jnp.broadcast_to(stat_in[n][:1], (sums.shape[-1], q)).T
        sums[n] = lax.rsqrt((sums[n] + theirs) * (1.0 / width) + EPS)

        @pl.loop(0, q // step)
        def _(t):
            rows = pl.ds(pl.multiple_of(t * step, step), step)
            z_ref[my_half, my_group + n, rows, :] = (held[n, rows, :] * sums[n, rows, :1] * gain[...]).astype(bf)

        piece, slot = piece_of((0, 0), n)
        for way in both(n % 2) + both(1 - n % 2):
            _send(piece, piece, gssem, gsem.at[slot], near[way])

    for n in range(side):
        matmul(n)
        first_hop(n)
        if n + 2 < side:
            pass_x(n + 2)
        if n > 0:
            second_hop(n - 1)
        if n > 2:
            norm(n - 3)
        if n > 1:
            add_up(n - 2)
    second_hop(side - 1)
    norm(side - 3)
    add_up(side - 2)
    add_up(side - 1)
    norm(side - 2)
    norm(side - 1)

    kept = [((0, 0), n) for n in range(side)]

    def take(k, n, ways):
        piece, slot = piece_of(k, n)
        _wait_recv(piece, gsem.at[slot], partner)
        for way in ways:
            _send(piece, piece, gssem, gsem.at[slot], near[way])
        if kept is None:
            _send(piece, piece, gssem, csem, partner)
        else:
            kept.append((k, n))

    def vec(n, d, e=0):
        return (d, e) if n % 2 == 0 else (e, d)

    def onward(n, axis, d):
        return ((axis, -d),) if (n < 2) == (d == -1) else ()

    def second(d1):
        for n in range(side):
            for d in (-1, 1):
                take(vec(n, d1, d), n, onward(n, 1 - n % 2, d))

    def far(d1):
        for n in range(side):
            take(vec(n, d1, 2), n, ())

    for n in range(side):
        for d in (-1, 1):
            take(vec(n, d), n, onward(n, n % 2, d) + both(1 - n % 2))

    _wait_send(z_ref.at[0, pl.ds(base, 7 * kg)], wssem, partner)
    _wait_send(x_wait_ref(0, side * side, 2), xrssem, partner)
    _wait_send(z_ref.at[1, pl.ds(base, 3 * side)], rssem, partner)
    pl.semaphore_signal(credit, inc=1, device_id={"tp": partner}, device_id_type=MESH)
    second(0)
    for n in range(side):
        take(vec(n, 2), n, both(1 - n % 2))
    pl.semaphore_wait(credit, 1)
    for k, n in kept:
        piece, _ = piece_of(k, n)
        _send(piece, piece, gssem, csem, partner)
    kept = None
    second(-1)
    second(1)
    far(0)
    second(2)
    far(-1)
    far(1)
    far(2)
    count = side * side * side
    _wait_recv(z_ref.at[0, pl.ds(0, count)], csem, partner)
    _wait_send(z_ref.at[:, pl.ds(0, count - side // 2)], gssem, partner)
    _wait_send(x_wait_ref(0, side * side, 5), xssem, partner)
    _wait_send(stat_out, tssem, partner)


def _store_kernel(z_ref, o_ref, sem):
    halves, groups, _, hw = z_ref.shape
    n = groups // 8
    copies = [
        pltpu.make_async_copy(
            z_ref.at[h, pl.ds(k * n, n)], o_ref.at[pl.ds(k * n, n), :, pl.ds(h * hw, hw)], sem.at[h, k])
        for k in range(8) for h in range(halves)
    ]
    for copy in copies:
        copy.start()
    for copy in copies:
        copy.wait()


def solution(mesh):
    tp = mesh.shape["tp"]
    side = math.isqrt(tp // CORES)

    def local(x, w, r, g):
        total, kf = x.shape
        width = w.shape[1]
        blk = total // tp
        bf = jnp.bfloat16
        dma = pltpu.SemaphoreType.DMA
        any_ = pl.BlockSpec(memory_space=pl.ANY)
        vmem = pl.BlockSpec(memory_space=pltpu.VMEM)
        q = blk // 2
        hw = width // 2
        groups = total // q
        z = pl.pallas_call(
            functools.partial(_fused_kernel, side),
            out_shape=pltpu.VMEM((2, groups, q, hw), bf),
            in_specs=[any_, any_, any_, vmem],
            out_specs=vmem,
            scratch_shapes=[
                pltpu.VMEM((side, side, q, CORES * kf), bf),
                pltpu.VMEM((2, side * q, hw), jnp.float32),
                pltpu.VMEM((side, q, hw), jnp.float32),
                pltpu.VMEM((1, hw), jnp.float32),
                pltpu.VMEM((side, q, 128), jnp.float32),
                pltpu.VMEM((side, 8, q), jnp.float32),
                pltpu.VMEM((side, 8, q), jnp.float32),
                dma((2 + side,)), dma((CORES,)), dma, dma,
                dma((side, CORES)), dma((side,)), dma, dma,
                dma((side, 4)), dma, dma((side,)), dma, pltpu.SemaphoreType.REGULAR,
                dma((side * side * side,)), dma, dma,
            ],
            compiler_params=pltpu.CompilerParams(
                collective_id=0, has_side_effects=True, vmem_limit_bytes=63 * 2**18),
            name="fused",
        )(x.reshape(CORES, 2, side, side * q, kf), w.reshape(kf // q, q, width), r.reshape(groups, q, width), g)
        out = pl.pallas_call(
            _store_kernel,
            out_shape=pltpu.HBM((groups, q, width), bf),
            in_specs=[vmem],
            out_specs=pl.BlockSpec(memory_space=pltpu.HBM),
            scratch_shapes=[dma((2, 8))],
            compiler_params=pltpu.CompilerParams(vmem_limit_bytes=2**20),
            name="store",
        )(z)
        return out.reshape(r.shape)

    return jax.shard_map(
        local,
        mesh=mesh,
        in_specs=(P("data", "tp"), P("tp", None), P("data", None), P(None)),
        out_specs=P("data", None),
        check_vma=False,
    )
```

```python
import functools
import math

import jax
import jax.numpy as jnp
from jax import lax
from jax.experimental import pallas as pl
from jax.experimental.pallas import tpu as pltpu
from jax.sharding import PartitionSpec as P

EPS = 1e-6
CORES = 2
PARTS = 4
MESH = pl.DeviceIdType.MESH


def _place(side):
    me = lax.axis_index("tp")
    c = lax.rem(me, CORES)
    chip = lax.div(me, CORES)
    xx, yy = lax.rem(chip, side), lax.div(chip, side)
    return me, c, xx + (yy - xx) * c, yy + (xx - yy) * c


def _dev(side, c, i, j):
    return CORES * (i * (1 + (side - 1) * c) + j * (side - (side - 1) * c)) + c


def _send(src, dst, ssem, rsem, dev):
    pltpu.make_async_remote_copy(
        src_ref=src, dst_ref=dst, send_sem=ssem, recv_sem=rsem,
        device_id={"tp": dev}, device_id_type=MESH,
    ).start()


def _wait_recv(ref, sem, dev):
    pltpu.make_async_remote_copy(
        src_ref=ref, dst_ref=ref, send_sem=sem, recv_sem=sem,
        device_id={"tp": dev}, device_id_type=MESH,
    ).wait_recv()


def _wait_send(ref, sem, dev):
    pltpu.make_async_remote_copy(
        src_ref=ref, dst_ref=ref, send_sem=sem, recv_sem=sem,
        device_id={"tp": dev}, device_id_type=MESH,
    ).wait_send()


def _barrier(devs):
    bar = pltpu.get_barrier_semaphore()
    for d in devs:
        pl.semaphore_signal(bar, inc=1, device_id={"tp": d}, device_id_type=MESH)
    pl.semaphore_wait(bar, len(devs))


def _fused_kernel(
    side, x_ref, w_ref, r_ref, g_ref, z_ref,
    xo, acc, held, gv, gain, sums, stat_out, stat_in,
    lsem, wrel, wsem, wssem, xrel, xsem, xssem, xrssem, rsem, rssem, tsem, tssem, credit, gsem, lsts, csem, gssem,
):
    me, c, i, j = _place(side)
    o = 1 - c
    halves, groups, q, hw = z_ref.shape
    width = halves * hw
    kf = x_ref.shape[-1]
    hq = q // 2
    kg = kf // q
    per_core = groups // CORES
    f32 = jnp.float32
    bf = z_ref.dtype

    def at(v, d):
        return lax.rem(v + d + side, side)

    def nh(a):
        return lax.div(a, side // 2)

    def mh(a):
        return lax.rem(lax.div(a + 1, 2), 2)

    def near_n(a):
        return a + 1 - 2 * lax.rem(a, 2)

    def near_m(a):
        return at(a, 2 * lax.rem(a, 2) - 1)

    jp, jm = at(j, 1), at(j, -1)
    partner = _dev(side, o, j, i)
    in_p, in_m = _dev(side, c, at(i, 1), j), _dev(side, c, at(i, -1), j)
    red_p, red_m = _dev(side, c, i, jp), _dev(side, c, i, jm)
    lines = []
    for cc, a, b in ((c, i, j), (o, j, i)):
        lines.append((cc, a, _dev(side, cc, near_n(a), b), _dev(side, cc, near_m(a), b)))
    from_p, from_m = _dev(side, o, j, at(i, 1)), _dev(side, o, j, at(i, -1))
    to_n, to_m = lines[0][2:]

    def cols_of(h):
        return pl.ds(pl.multiple_of(h * hw, hw), hw)

    def lent(cc, half, first, size):
        return half, pl.ds((1 - cc) * per_core + first, size)

    def w_at(cc, role, core):
        h, g = lent(cc, 0, (role * CORES + core) * kg, kg)
        return z_ref.at[h, g]

    x_first = side * CORES * kg

    def x_at(cc, n, role, core):
        if role == 3:
            return xo.at[n, :, :, pl.ds(core * kf, kf)]
        h, g = lent(cc, 0, x_first + n * side, side)
        return z_ref.at[h, g, :, pl.ds((role * CORES + core) * kf, kf)]

    names = ("s2", "sp", "sm", "fm", "fp", "ra", "rb")
    base = o * per_core

    def buf(k, n):
        return base + names.index(k) * side + n

    def own_group(ii, jj):
        return nh(ii), ((c * 2 + mh(ii)) * side + jj) * side

    my_half, my_group = own_group(i, j)

    cw = pltpu.make_async_copy(w_ref.at[:, :, cols_of(nh(i))], w_at(c, 0, c), lsem.at[0])
    cw.start()
    cr = pltpu.make_async_copy(
        r_ref.at[pl.ds(my_group, side), :, cols_of(nh(i))], z_ref.at[my_half, pl.ds(my_group, side)], lsem.at[1])
    cr.start()
    cg = pltpu.make_async_copy(g_ref, gv, lsem.at[2 + side])
    cg.start()
    cx = [pltpu.make_async_copy(x_ref.at[c, mh(i), :, pl.ds(n * q, q)], x_at(c, n, 0, c), lsem.at[2 + n])
          for n in range(side)]
    for copy in cx:
        copy.start()

    _barrier((partner, in_p, in_m, red_p, red_m, lines[1][2], lines[1][3], from_p, from_m))

    for cc, a, dev_n, dev_m in lines:
        _send(w_ref.at[:, :, cols_of(1 - nh(a))], w_at(cc, 2, c), wssem, wrel.at[c], dev_m)
    for cc, a, dev_n, dev_m in lines:
        _send(w_ref.at[:, :, cols_of(nh(a))], w_at(cc, 1, c), wssem, wsem, dev_n)
    _send(w_ref.at[:, :, cols_of(nh(j))], w_at(o, 0, c), wssem, wsem, partner)

    def send_x(n):
        rows = pl.ds(n * q, q)
        for cc, a, dev_n, dev_m in lines:
            _send(x_ref.at[cc, mh(a), :, rows], x_at(cc, n, 2, c), xssem, xsem.at[n], dev_m)
        _send(x_ref.at[o, mh(j), :, rows], x_at(o, n, 0, c), xssem, xsem.at[n], partner)

    def relay_x(n, line):
        cc, a, dev_n, dev_m = line
        _send(x_ref.at[cc, 1 - mh(a), :, pl.ds(n * q, q)], x_at(cc, n, 1, c), xssem, xrel.at[n, c], dev_n)

    def pass_x(n):
        for e in range(CORES):
            piece = x_at(c, n, 1, e)
            _wait_recv(piece, xrel.at[n, e], partner)
            _send(piece, x_at(c, n, 3, e), xrssem, xsem.at[n], to_m)

    cg.wait()
    gain[...] = jnp.where(
        my_half == 0, gv[...].astype(f32).reshape(1, width)[:, :hw], gv[...].astype(f32).reshape(1, width)[:, hw:])

    def pass_w(e):
        piece = w_at(c, 2, e)
        _wait_recv(piece, wrel.at[e], partner)
        _send(piece, w_at(c, 3, e), wssem, wsem, to_n)

    for n in range(side):
        send_x(n)
    for line in lines:
        relay_x(0, line)
    pass_w(0)
    pass_w(1)
    for line in lines:
        relay_x(1, line)
    pass_x(0)
    for line in lines:
        relay_x(2, line)
    pass_x(1)
    for line in lines:
        relay_x(3, line)
    pass_x(2)
    pass_x(3)
    _wait_recv(z_ref.at[0, pl.ds(base, 5 * kg)], wsem, partner)
    cw.wait()

    tile = next(t for t in (512, 256, 128) if hw % t == 0)
    step = next(t for t in (32, 16, 8) if hq % t == 0)
    roles = 3 * CORES

    def x_wait_ref(first, size, pieces):
        return z_ref.at[0, pl.ds(base + x_first + first, size), :, pl.ds(0, pieces * kf)]

    def matmul(n):
        cx[n].wait()
        _wait_recv(x_wait_ref(n * side, side, 5), xsem.at[n], partner)

        @pl.loop(0, hw // tile)
        def _(t):
            cols = pl.ds(pl.multiple_of(t * tile, tile), tile)
            near = jnp.dot(
                z_ref[0, pl.ds(base + x_first + n * side, side), :, pl.ds(0, roles * kf)].reshape(side * q, roles * kf),
                z_ref[0, pl.ds(base, roles * kg), :, cols].reshape(roles * kf, tile), preferred_element_type=f32)
            acc[n % 2, :, cols] = near + jnp.dot(
                xo[n].reshape(side * q, CORES * kf),
                z_ref[0, pl.ds(base + roles * kg, CORES * kg), :, cols].reshape(CORES * kf, tile),
                preferred_element_type=f32)

    def part(n, block, first, size):
        return acc.at[n % 2, pl.ds(pl.multiple_of(block * q, q) + first, size)]

    def send_part(n, k, block, first, add, dst, sem, dev):
        src = part(n, block, first, hq)

        @pl.loop(0, hq // step)
        def _(t):
            off = pl.multiple_of(t * step, step)
            v = src[pl.ds(off, step), :]
            if add is not None:
                v = v + z_ref[1, buf(add, n), pl.ds(off, step), :].astype(f32)
            z_ref[1, buf(k, n), pl.ds(first + off, step), :] = v.astype(bf)

        to = 0 if dst in ("ra", "rb") else first
        _send(z_ref.at[1, buf(k, n), pl.ds(first, hq)], z_ref.at[1, buf(dst, n), pl.ds(to, hq)], rssem, sem, dev)

    def first_hop(n):
        send_part(n, "s2", at(j, 2), 0, None, "ra", rsem.at[n, 0], red_p)
        send_part(n, "s2", at(j, 2), hq, None, "rb", rsem.at[n, 1], red_m)
        send_part(n, "sp", jp, hq, None, "fm", rsem.at[n, 2], red_p)
        send_part(n, "sm", jm, 0, None, "fp", rsem.at[n, 3], red_m)
        src = part(n, j, 0, q)

        @pl.loop(0, q // step)
        def _(t):
            rows = pl.ds(pl.multiple_of(t * step, step), step)
            held[n, rows, :] = src[rows, :]

    def second_hop(n):
        _wait_recv(z_ref.at[1, buf("ra", n), pl.ds(0, hq)], rsem.at[n, 0], partner)
        send_part(n, "sp", jp, 0, "ra", "fm", rsem.at[n, 2], red_p)
        _wait_recv(z_ref.at[1, buf("rb", n), pl.ds(0, hq)], rsem.at[n, 1], partner)
        send_part(n, "sm", jm, hq, "rb", "fp", rsem.at[n, 3], red_m)

    def add_up(n):
        if n == 0:
            cr.wait()
        _wait_recv(z_ref.at[1, buf("fm", n)], rsem.at[n, 2], partner)
        _wait_recv(z_ref.at[1, buf("fp", n)], rsem.at[n, 3], partner)

        @pl.loop(0, q // step)
        def _(t):
            rows = pl.ds(pl.multiple_of(t * step, step), step)
            y = held[n, rows, :] + (
                z_ref[1, buf("fm", n), rows, :].astype(f32) + z_ref[1, buf("fp", n), rows, :].astype(f32))
            v = z_ref[my_half, my_group + n, rows, :].astype(f32) + y.astype(bf).astype(f32)
            held[n, rows, :] = v
            sums[n, rows, :] = jnp.broadcast_to(jnp.sum(v * v, axis=-1, keepdims=True), (step, sums.shape[-1]))

        stat_out[n] = sums[n].T[:8]
        _send(stat_out.at[n], stat_in.at[n], tssem, tsem.at[n], to_m)

    near = {(0, 1): in_p, (0, -1): in_m, (1, 1): red_p, (1, -1): red_m}

    def piece_of(k, n):
        ii, jj = at(i, k[0]), at(j, k[1])
        h, g = own_group(ii, jj)
        return z_ref.at[h, g + n], (ii * side + jj) * side + n

    def both(axis):
        return (axis, 1), (axis, -1)

    def norm(n):
        _wait_recv(stat_in.at[n], tsem.at[n], partner)
        theirs = jnp.broadcast_to(stat_in[n][:1], (sums.shape[-1], q)).T
        sums[n] = lax.rsqrt((sums[n] + theirs) * (1.0 / width) + EPS)

        @pl.loop(0, q // step)
        def _(t):
            rows = pl.ds(pl.multiple_of(t * step, step), step)
            z_ref[my_half, my_group + n, rows, :] = (held[n, rows, :] * sums[n, rows, :1] * gain[...]).astype(bf)

        piece, slot = piece_of((0, 0), n)
        for way in both(n % 2) + both(1 - n % 2):
            _send(piece, piece, gssem, gsem.at[slot], near[way])

    for n in range(side):
        matmul(n)
        first_hop(n)
        if n > 0:
            second_hop(n - 1)
        if n > 2:
            norm(n - 3)
        if n > 1:
            add_up(n - 2)
    second_hop(side - 1)
    norm(side - 3)
    add_up(side - 2)
    add_up(side - 1)
    norm(side - 2)
    norm(side - 1)

    kept = [((0, 0), n) for n in range(side)]

    size = q // PARTS

    def take(k, n, ways, last=False):
        piece, slot = piece_of(k, n)
        _wait_recv(piece, gsem.at[slot], partner)
        for way in ways:
            if last:
                for m in range(PARTS):
                    bit = piece.at[pl.ds(m * size, size)]
                    _send(bit, bit, gssem, lsts.at[n, m], near[way])
            else:
                _send(piece, piece, gssem, gsem.at[slot], near[way])
        if kept is None:
            _send(piece, piece, gssem, csem, partner)
        else:
            kept.append((k, n))

    def vec(n, d, e=0):
        return (d, e) if n % 2 == 0 else (e, d)

    def onward(n, axis, d):
        return ((axis, -d),) if (n < 2) == (d == -1) else ()

    def second(d1):
        for n in range(side):
            for d in (-1, 1):
                take(vec(n, d1, d), n, onward(n, 1 - n % 2, d), d1 == 2)

    def far(d1):
        for n in range(side):
            take(vec(n, d1, 2), n, ())

    for n in range(side):
        for d in (-1, 1):
            take(vec(n, d), n, onward(n, n % 2, d) + both(1 - n % 2))

    _wait_send(z_ref.at[0, pl.ds(base, 7 * kg)], wssem, partner)
    _wait_send(x_wait_ref(0, side * side, 2), xrssem, partner)
    _wait_send(z_ref.at[1, pl.ds(base, 3 * side)], rssem, partner)
    pl.semaphore_signal(credit, inc=1, device_id={"tp": partner}, device_id_type=MESH)
    second(0)
    for n in range(side):
        take(vec(n, 2), n, both(1 - n % 2))
    pl.semaphore_wait(credit, 1)
    for k, n in kept:
        piece, _ = piece_of(k, n)
        _send(piece, piece, gssem, csem, partner)
    kept = None
    second(-1)
    second(1)
    far(0)
    second(2)
    far(-1)
    far(1)
    for m in range(PARTS):
        for n in range(side):
            bit = piece_of(vec(n, 2, 2), n)[0].at[pl.ds(m * size, size)]
            _wait_recv(bit, lsts.at[n, m], partner)
            _send(bit, bit, gssem, csem, partner)
    count = side * side * side
    _wait_recv(z_ref.at[0, pl.ds(0, count)], csem, partner)
    _wait_send(z_ref.at[:, pl.ds(0, count - side // 2)], gssem, partner)
    _wait_send(x_wait_ref(0, side * side, 5), xssem, partner)
    _wait_send(stat_out, tssem, partner)


def _store_kernel(z_ref, o_ref, sem):
    halves, groups, _, hw = z_ref.shape
    n = groups // 8
    copies = [
        pltpu.make_async_copy(
            z_ref.at[h, pl.ds(k * n, n)], o_ref.at[pl.ds(k * n, n), :, pl.ds(h * hw, hw)], sem.at[h, k])
        for k in range(8) for h in range(halves)
    ]
    for copy in copies:
        copy.start()
    for copy in copies:
        copy.wait()


def solution(mesh):
    tp = mesh.shape["tp"]
    side = math.isqrt(tp // CORES)

    def local(x, w, r, g):
        total, kf = x.shape
        width = w.shape[1]
        blk = total // tp
        bf = jnp.bfloat16
        dma = pltpu.SemaphoreType.DMA
        any_ = pl.BlockSpec(memory_space=pl.ANY)
        vmem = pl.BlockSpec(memory_space=pltpu.VMEM)
        q = blk // 2
        hw = width // 2
        groups = total // q
        z = pl.pallas_call(
            functools.partial(_fused_kernel, side),
            out_shape=pltpu.VMEM((2, groups, q, hw), bf),
            in_specs=[any_, any_, any_, any_],
            out_specs=vmem,
            scratch_shapes=[
                pltpu.VMEM((side, side, q, CORES * kf), bf),
                pltpu.VMEM((2, side * q, hw), jnp.float32),
                pltpu.VMEM((side, q, hw), jnp.float32),
                pltpu.VMEM((width,), bf),
                pltpu.VMEM((1, hw), jnp.float32),
                pltpu.VMEM((side, q, 128), jnp.float32),
                pltpu.VMEM((side, 8, q), jnp.float32),
                pltpu.VMEM((side, 8, q), jnp.float32),
                dma((3 + side,)), dma((CORES,)), dma, dma,
                dma((side, CORES)), dma((side,)), dma, dma,
                dma((side, 4)), dma, dma((side,)), dma, pltpu.SemaphoreType.REGULAR,
                dma((side * side * side,)), dma((side, PARTS)), dma, dma,
            ],
            compiler_params=pltpu.CompilerParams(
                collective_id=0, has_side_effects=True, vmem_limit_bytes=63 * 2**18),
            name="fused",
        )(x.reshape(CORES, 2, side, side * q, kf), w.reshape(kf // q, q, width), r.reshape(groups, q, width), g)
        out = pl.pallas_call(
            _store_kernel,
            out_shape=pltpu.HBM((groups, q, width), bf),
            in_specs=[vmem],
            out_specs=pl.BlockSpec(memory_space=pltpu.HBM),
            scratch_shapes=[dma((2, 8))],
            compiler_params=pltpu.CompilerParams(vmem_limit_bytes=2**20),
            name="store",
        )(z)
        return out.reshape(r.shape)

    return jax.shard_map(
        local,
        mesh=mesh,
        in_specs=(P("data", "tp"), P("tp", None), P("data", None), P(None)),
        out_specs=P("data", None),
        check_vma=False,
    )
```

```python
import functools
import math

import jax
import jax.numpy as jnp
from jax import lax
from jax.experimental import pallas as pl
from jax.experimental.pallas import tpu as pltpu
from jax.sharding import PartitionSpec as P

EPS = 1e-6
CORES = 2
PARTS = 8
MESH = pl.DeviceIdType.MESH


def _place(side):
    me = lax.axis_index("tp")
    c = lax.rem(me, CORES)
    chip = lax.div(me, CORES)
    xx, yy = lax.rem(chip, side), lax.div(chip, side)
    return me, c, xx + (yy - xx) * c, yy + (xx - yy) * c


def _dev(side, c, i, j):
    return CORES * (i * (1 + (side - 1) * c) + j * (side - (side - 1) * c)) + c


def _send(src, dst, ssem, rsem, dev):
    pltpu.make_async_remote_copy(
        src_ref=src, dst_ref=dst, send_sem=ssem, recv_sem=rsem,
        device_id={"tp": dev}, device_id_type=MESH,
    ).start()


def _wait_recv(ref, sem, dev):
    pltpu.make_async_remote_copy(
        src_ref=ref, dst_ref=ref, send_sem=sem, recv_sem=sem,
        device_id={"tp": dev}, device_id_type=MESH,
    ).wait_recv()


def _wait_send(ref, sem, dev):
    pltpu.make_async_remote_copy(
        src_ref=ref, dst_ref=ref, send_sem=sem, recv_sem=sem,
        device_id={"tp": dev}, device_id_type=MESH,
    ).wait_send()


def _barrier(devs):
    bar = pltpu.get_barrier_semaphore()
    for d in devs:
        pl.semaphore_signal(bar, inc=1, device_id={"tp": d}, device_id_type=MESH)
    pl.semaphore_wait(bar, len(devs))


def _fused_kernel(
    side, x_ref, w_ref, r_ref, g_ref, z_ref,
    xo, acc, held, gv, gain, sums, stat_out, stat_in,
    lsem, wrel, wsem, wssem, xrel, xsem, xssem, xrssem, rsem, rssem, tsem, tssem, credit, gsem, lsts, csem, gssem,
):
    me, c, i, j = _place(side)
    o = 1 - c
    halves, groups, q, hw = z_ref.shape
    width = halves * hw
    kf = x_ref.shape[-1]
    hq = q // 2
    kg = kf // q
    per_core = groups // CORES
    f32 = jnp.float32
    bf = z_ref.dtype

    def at(v, d):
        return lax.rem(v + d + side, side)

    def nh(a):
        return lax.div(a, side // 2)

    def mh(a):
        return lax.rem(lax.div(a + 1, 2), 2)

    def near_n(a):
        return a + 1 - 2 * lax.rem(a, 2)

    def near_m(a):
        return at(a, 2 * lax.rem(a, 2) - 1)

    jp, jm = at(j, 1), at(j, -1)
    partner = _dev(side, o, j, i)
    in_p, in_m = _dev(side, c, at(i, 1), j), _dev(side, c, at(i, -1), j)
    red_p, red_m = _dev(side, c, i, jp), _dev(side, c, i, jm)
    lines = []
    for cc, a, b in ((c, i, j), (o, j, i)):
        lines.append((cc, a, _dev(side, cc, near_n(a), b), _dev(side, cc, near_m(a), b)))
    from_p, from_m = _dev(side, o, j, at(i, 1)), _dev(side, o, j, at(i, -1))
    to_n, to_m = lines[0][2:]

    def cols_of(h):
        return pl.ds(pl.multiple_of(h * hw, hw), hw)

    def lent(cc, half, first, size):
        return half, pl.ds((1 - cc) * per_core + first, size)

    def w_at(cc, role, core):
        h, g = lent(cc, 0, (role * CORES + core) * kg, kg)
        return z_ref.at[h, g]

    x_first = side * CORES * kg

    def x_at(cc, n, role, core):
        if role == 3:
            return xo.at[n, :, :, pl.ds(core * kf, kf)]
        h, g = lent(cc, 0, x_first + n * side, side)
        return z_ref.at[h, g, :, pl.ds((role * CORES + core) * kf, kf)]

    names = ("s2", "sp", "sm", "fm", "fp", "ra", "rb")
    base = o * per_core

    def buf(k, n):
        return base + names.index(k) * side + n

    def own_group(ii, jj):
        return nh(ii), ((c * 2 + mh(ii)) * side + jj) * side

    my_half, my_group = own_group(i, j)

    cw = pltpu.make_async_copy(w_ref.at[:, :, cols_of(nh(i))], w_at(c, 0, c), lsem.at[0])
    cw.start()
    cr = pltpu.make_async_copy(
        r_ref.at[pl.ds(my_group, side), :, cols_of(nh(i))], z_ref.at[my_half, pl.ds(my_group, side)], lsem.at[1])
    cr.start()
    cg = pltpu.make_async_copy(g_ref, gv, lsem.at[2 + side])
    cg.start()
    cx = [pltpu.make_async_copy(x_ref.at[c, mh(i), :, pl.ds(n * q, q)], x_at(c, n, 0, c), lsem.at[2 + n])
          for n in range(side)]
    for copy in cx:
        copy.start()

    _barrier((partner, in_p, in_m, red_p, red_m, lines[1][2], lines[1][3], from_p, from_m))

    for cc, a, dev_n, dev_m in lines:
        _send(w_ref.at[:, :, cols_of(1 - nh(a))], w_at(cc, 2, c), wssem, wrel.at[c], dev_m)
    for cc, a, dev_n, dev_m in lines:
        _send(w_ref.at[:, :, cols_of(nh(a))], w_at(cc, 1, c), wssem, wsem, dev_n)
    _send(w_ref.at[:, :, cols_of(nh(j))], w_at(o, 0, c), wssem, wsem, partner)

    def send_x(n):
        rows = pl.ds(n * q, q)
        for cc, a, dev_n, dev_m in lines:
            _send(x_ref.at[cc, mh(a), :, rows], x_at(cc, n, 2, c), xssem, xsem.at[n], dev_m)
        _send(x_ref.at[o, mh(j), :, rows], x_at(o, n, 0, c), xssem, xsem.at[n], partner)

    def relay_x(n, line):
        cc, a, dev_n, dev_m = line
        _send(x_ref.at[cc, 1 - mh(a), :, pl.ds(n * q, q)], x_at(cc, n, 1, c), xssem, xrel.at[n, c], dev_n)

    def pass_x(n):
        for e in range(CORES):
            piece = x_at(c, n, 1, e)
            _wait_recv(piece, xrel.at[n, e], partner)
            _send(piece, x_at(c, n, 3, e), xrssem, xsem.at[n], to_m)

    cg.wait()
    gain[...] = jnp.where(
        my_half == 0, gv[...].astype(f32).reshape(1, width)[:, :hw], gv[...].astype(f32).reshape(1, width)[:, hw:])

    def pass_w(e):
        piece = w_at(c, 2, e)
        _wait_recv(piece, wrel.at[e], partner)
        _send(piece, w_at(c, 3, e), wssem, wsem, to_n)

    for n in range(side):
        send_x(n)
    for line in lines:
        relay_x(0, line)
    pass_w(0)
    pass_w(1)
    for line in lines:
        relay_x(1, line)
    pass_x(0)
    for line in lines:
        relay_x(2, line)
    pass_x(1)
    for line in lines:
        relay_x(3, line)
    pass_x(2)
    pass_x(3)
    _wait_recv(z_ref.at[0, pl.ds(base, 5 * kg)], wsem, partner)
    cw.wait()

    tile = next(t for t in (512, 256, 128) if hw % t == 0)
    step = next(t for t in (32, 16, 8) if hq % t == 0)
    roles = 3 * CORES

    def x_wait_ref(first, size, pieces):
        return z_ref.at[0, pl.ds(base + x_first + first, size), :, pl.ds(0, pieces * kf)]

    def matmul(n):
        cx[n].wait()
        _wait_recv(x_wait_ref(n * side, side, 5), xsem.at[n], partner)

        @pl.loop(0, hw // tile)
        def _(t):
            cols = pl.ds(pl.multiple_of(t * tile, tile), tile)
            near = jnp.dot(
                z_ref[0, pl.ds(base + x_first + n * side, side), :, pl.ds(0, roles * kf)].reshape(side * q, roles * kf),
                z_ref[0, pl.ds(base, roles * kg), :, cols].reshape(roles * kf, tile), preferred_element_type=f32)
            acc[n % 2, :, cols] = near + jnp.dot(
                xo[n].reshape(side * q, CORES * kf),
                z_ref[0, pl.ds(base + roles * kg, CORES * kg), :, cols].reshape(CORES * kf, tile),
                preferred_element_type=f32)

    def part(n, block, first, size):
        return acc.at[n % 2, pl.ds(pl.multiple_of(block * q, q) + first, size)]

    def send_part(n, k, block, first, add, dst, sem, dev):
        src = part(n, block, first, hq)

        @pl.loop(0, hq // step)
        def _(t):
            off = pl.multiple_of(t * step, step)
            v = src[pl.ds(off, step), :]
            if add is not None:
                v = v + z_ref[1, buf(add, n), pl.ds(off, step), :].astype(f32)
            z_ref[1, buf(k, n), pl.ds(first + off, step), :] = v.astype(bf)

        to = 0 if dst in ("ra", "rb") else first
        _send(z_ref.at[1, buf(k, n), pl.ds(first, hq)], z_ref.at[1, buf(dst, n), pl.ds(to, hq)], rssem, sem, dev)

    def first_hop(n):
        send_part(n, "s2", at(j, 2), 0, None, "ra", rsem.at[n, 0], red_p)
        send_part(n, "s2", at(j, 2), hq, None, "rb", rsem.at[n, 1], red_m)
        send_part(n, "sp", jp, hq, None, "fm", rsem.at[n, 2], red_p)
        send_part(n, "sm", jm, 0, None, "fp", rsem.at[n, 3], red_m)
        src = part(n, j, 0, q)

        @pl.loop(0, q // step)
        def _(t):
            rows = pl.ds(pl.multiple_of(t * step, step), step)
            held[n, rows, :] = src[rows, :]

    def second_hop(n):
        _wait_recv(z_ref.at[1, buf("ra", n), pl.ds(0, hq)], rsem.at[n, 0], partner)
        send_part(n, "sp", jp, 0, "ra", "fm", rsem.at[n, 2], red_p)
        _wait_recv(z_ref.at[1, buf("rb", n), pl.ds(0, hq)], rsem.at[n, 1], partner)
        send_part(n, "sm", jm, hq, "rb", "fp", rsem.at[n, 3], red_m)

    def add_up(n):
        if n == 0:
            cr.wait()
        _wait_recv(z_ref.at[1, buf("fm", n)], rsem.at[n, 2], partner)
        _wait_recv(z_ref.at[1, buf("fp", n)], rsem.at[n, 3], partner)

        @pl.loop(0, q // step)
        def _(t):
            rows = pl.ds(pl.multiple_of(t * step, step), step)
            y = held[n, rows, :] + (
                z_ref[1, buf("fm", n), rows, :].astype(f32) + z_ref[1, buf("fp", n), rows, :].astype(f32))
            v = z_ref[my_half, my_group + n, rows, :].astype(f32) + y.astype(bf).astype(f32)
            held[n, rows, :] = v
            sums[n, rows, :] = jnp.broadcast_to(jnp.sum(v * v, axis=-1, keepdims=True), (step, sums.shape[-1]))

        stat_out[n] = sums[n].T[:8]
        _send(stat_out.at[n], stat_in.at[n], tssem, tsem.at[n], to_m)

    near = {(0, 1): in_p, (0, -1): in_m, (1, 1): red_p, (1, -1): red_m}

    def piece_of(k, n):
        ii, jj = at(i, k[0]), at(j, k[1])
        h, g = own_group(ii, jj)
        return z_ref.at[h, g + n], (ii * side + jj) * side + n

    def both(axis):
        return (axis, 1), (axis, -1)

    def norm(n):
        _wait_recv(stat_in.at[n], tsem.at[n], partner)
        theirs = jnp.broadcast_to(stat_in[n][:1], (sums.shape[-1], q)).T
        sums[n] = lax.rsqrt((sums[n] + theirs) * (1.0 / width) + EPS)

        @pl.loop(0, q // step)
        def _(t):
            rows = pl.ds(pl.multiple_of(t * step, step), step)
            z_ref[my_half, my_group + n, rows, :] = (held[n, rows, :] * sums[n, rows, :1] * gain[...]).astype(bf)

        piece, slot = piece_of((0, 0), n)
        for way in both(n % 2) + both(1 - n % 2):
            _send(piece, piece, gssem, gsem.at[slot], near[way])

    for n in range(side):
        matmul(n)
        first_hop(n)
        if n > 0:
            second_hop(n - 1)
        if n > 2:
            norm(n - 3)
        if n > 1:
            add_up(n - 2)
    second_hop(side - 1)
    norm(side - 3)
    add_up(side - 2)
    add_up(side - 1)
    norm(side - 2)
    norm(side - 1)

    kept = [((0, 0), n) for n in range(side)]

    size = q // PARTS

    def take(k, n, ways, last=False):
        piece, slot = piece_of(k, n)
        _wait_recv(piece, gsem.at[slot], partner)
        for way in ways:
            if last:
                for m in range(PARTS):
                    bit = piece.at[pl.ds(m * size, size)]
                    _send(bit, bit, gssem, lsts.at[n, m], near[way])
            else:
                _send(piece, piece, gssem, gsem.at[slot], near[way])
        if kept is None:
            _send(piece, piece, gssem, csem, partner)
        else:
            kept.append((k, n))

    def vec(n, d, e=0):
        return (d, e) if n % 2 == 0 else (e, d)

    def onward(n, axis, d):
        return ((axis, -d),) if (n < 2) == (d == -1) else ()

    def second(d1):
        for n in range(side):
            for d in (-1, 1):
                take(vec(n, d1, d), n, onward(n, 1 - n % 2, d), d1 == 2)

    def far(d1):
        for n in range(side):
            take(vec(n, d1, 2), n, ())

    for n in range(side):
        for d in (-1, 1):
            take(vec(n, d), n, onward(n, n % 2, d) + both(1 - n % 2))

    _wait_send(z_ref.at[0, pl.ds(base, 7 * kg)], wssem, partner)
    _wait_send(x_wait_ref(0, side * side, 2), xrssem, partner)
    _wait_send(z_ref.at[1, pl.ds(base, 3 * side)], rssem, partner)
    pl.semaphore_signal(credit, inc=1, device_id={"tp": partner}, device_id_type=MESH)
    second(0)
    for n in range(side):
        take(vec(n, 2), n, both(1 - n % 2))
    pl.semaphore_wait(credit, 1)
    for k, n in kept:
        piece, _ = piece_of(k, n)
        _send(piece, piece, gssem, csem, partner)
    kept = None
    second(-1)
    second(1)
    far(0)
    second(2)
    far(-1)
    far(1)
    for m in range(PARTS):
        for n in range(side):
            bit = piece_of(vec(n, 2, 2), n)[0].at[pl.ds(m * size, size)]
            _wait_recv(bit, lsts.at[n, m], partner)
            _send(bit, bit, gssem, csem, partner)
    count = side * side * side
    _wait_recv(z_ref.at[0, pl.ds(0, count)], csem, partner)
    _wait_send(z_ref.at[:, pl.ds(0, count - side // 2)], gssem, partner)
    _wait_send(x_wait_ref(0, side * side, 5), xssem, partner)
    _wait_send(stat_out, tssem, partner)


def _store_kernel(z_ref, o_ref, sem):
    halves, groups, _, hw = z_ref.shape
    n = groups // 8
    copies = [
        pltpu.make_async_copy(
            z_ref.at[h, pl.ds(k * n, n)], o_ref.at[pl.ds(k * n, n), :, pl.ds(h * hw, hw)], sem.at[h, k])
        for k in range(8) for h in range(halves)
    ]
    for copy in copies:
        copy.start()
    for copy in copies:
        copy.wait()


def solution(mesh):
    tp = mesh.shape["tp"]
    side = math.isqrt(tp // CORES)

    def local(x, w, r, g):
        total, kf = x.shape
        width = w.shape[1]
        blk = total // tp
        bf = jnp.bfloat16
        dma = pltpu.SemaphoreType.DMA
        any_ = pl.BlockSpec(memory_space=pl.ANY)
        vmem = pl.BlockSpec(memory_space=pltpu.VMEM)
        q = blk // 2
        hw = width // 2
        groups = total // q
        z = pl.pallas_call(
            functools.partial(_fused_kernel, side),
            out_shape=pltpu.VMEM((2, groups, q, hw), bf),
            in_specs=[any_, any_, any_, any_],
            out_specs=vmem,
            scratch_shapes=[
                pltpu.VMEM((side, side, q, CORES * kf), bf),
                pltpu.VMEM((2, side * q, hw), jnp.float32),
                pltpu.VMEM((side, q, hw), jnp.float32),
                pltpu.VMEM((width,), bf),
                pltpu.VMEM((1, hw), jnp.float32),
                pltpu.VMEM((side, q, 128), jnp.float32),
                pltpu.VMEM((side, 8, q), jnp.float32),
                pltpu.VMEM((side, 8, q), jnp.float32),
                dma((3 + side,)), dma((CORES,)), dma, dma,
                dma((side, CORES)), dma((side,)), dma, dma,
                dma((side, 4)), dma, dma((side,)), dma, pltpu.SemaphoreType.REGULAR,
                dma((side * side * side,)), dma((side, PARTS)), dma, dma,
            ],
            compiler_params=pltpu.CompilerParams(
                collective_id=0, has_side_effects=True, vmem_limit_bytes=63 * 2**18),
            name="fused",
        )(x.reshape(CORES, 2, side, side * q, kf), w.reshape(kf // q, q, width), r.reshape(groups, q, width), g)
        out = pl.pallas_call(
            _store_kernel,
            out_shape=pltpu.HBM((groups, q, width), bf),
            in_specs=[vmem],
            out_specs=pl.BlockSpec(memory_space=pltpu.HBM),
            scratch_shapes=[dma((2, 8))],
            compiler_params=pltpu.CompilerParams(vmem_limit_bytes=2**20),
            name="store",
        )(z)
        return out.reshape(r.shape)

    return jax.shard_map(
        local,
        mesh=mesh,
        in_specs=(P("data", "tp"), P("tp", None), P("data", None), P(None)),
        out_specs=P("data", None),
        check_vma=False,
    )
```
